32 devices in a mesh: dp: 2 (over x), vocab: 16 (over z, y, core).
Axes of the slice: x: 2, y: 2, z: 4, core: 2. Of those that a mesh axis runs over, the one named last changes fastest.
Arguments:
- hidden: bfloat16 [448, 4608], P('dp'), may hold values from -15 to 15
- out_weight: bfloat16 [4608, 6144], P('dp', 'vocab'), may hold values from -0.09375 to 0.09375
- targets: int32 [448], P('dp'), may hold values from 0 to 5951
- token_weight: float32 [448], P('dp'), may hold values from 0.3 to 3
Outputs:
- token_loss: float32 [448], P('dp')
- hidden_grad: bfloat16 [448, 4608], P('dp')
- weight_grad: bfloat16 [4608, 6144], P('dp', 'vocab')
The draws below stay inside these ranges and needn't reach their ends.
All inputs are finite; a program needn't handle non-finite values.
Results may differ from the reference program's by a relative error of at most 0.0085.
Values may be sent and summed in bfloat16 or wider, within the bound.
A program may use at most 64 MiB of HBM per device.

```python
import math
import jax
import jax.numpy as jnp
from jax import lax

D = 4608
VOCAB_DEV = 384
TOK_DEV = 224
TOKENS = 448
VOCAB_PAD = 6144
VOCAB = 5952
N_DP = 2
N_VOCAB = 16


def touch_ends(drawn, own_key, smallest, largest):
    index_at = [jax.random.randint(jax.random.fold_in(own_key, axis), (), 0, length) for axis, length in enumerate(drawn.shape)]
    longest = drawn.shape.index(max(drawn.shape))
    beside = index_at[:longest] + [(index_at[longest] + 1) % drawn.shape[longest]] + index_at[longest + 1:]
    return drawn.at[tuple(index_at)].set(smallest).at[tuple(beside)].set(largest)


def block_scale(own_key, shape, cuts, smallest, high):
    factor_of = 1.0
    for position, shards_of in cuts:
        steps = jax.random.uniform(jax.random.fold_in(jax.random.fold_in(own_key, 6), position), (shards_of,), jnp.float32, smallest / len(cuts), high / len(cuts))
        factor_of = factor_of * jnp.repeat(jnp.exp(steps), shape[position] // shards_of).reshape((-1,) + (1,) * (len(shape) - 1 - position))
    return factor_of


def gaussian(rng, dims, width, limit, shards=(), held_as=jnp.bfloat16):
    drawn = jax.random.normal(rng, dims, jnp.float32) * width
    if len(shards) > 0:
        drawn = block_scale(rng, dims, shards, -0.22, 0.18) * drawn
    return jnp.clip(drawn, min=-limit, max=limit).astype(held_as)


def setup_inputs(seed: int = 0) -> dict:
    streams_of = jax.random.split(jax.random.key(seed), 5)
    hidden = gaussian(streams_of[0], (TOKENS, D), 3.0, 15.0, ((0, 2),))
    out_weight = gaussian(streams_of[1], (D, VOCAB_PAD), D ** -0.5, 0.09375, ((0, 2), (1, 16)))
    targets = touch_ends(jax.random.randint(streams_of[2], (TOKENS,), 0, VOCAB), jax.random.fold_in(streams_of[2], 1), 0, VOCAB - 1).astype(jnp.int32)
    token_weight = jnp.clip(jnp.exp(math.log(3.0) - 2.3025851 * jax.random.uniform(streams_of[3], (TOKENS,), jnp.float32) ** block_scale(streams_of[3], (TOKENS,), ((0, 2),), -0.2, 0.2)), 0.3, 3.0)
    return dict(hidden=hidden, out_weight=out_weight, targets=targets, token_weight=token_weight)


softcap = 30.0


def reference(hidden, out_weight, targets, token_weight):
    padded = VOCAB_DEV * N_VOCAB
    logits = jnp.dot(hidden, out_weight, preferred_element_type=jnp.float32)
    squash = jnp.tanh(logits / softcap)
    capped = softcap * squash
    col_ids = jnp.arange(padded, dtype=jnp.int32)
    usable = col_ids < VOCAB
    exp_terms = jnp.where(usable[None, :], jnp.exp(capped), jnp.float32(0.0))
    sums = jnp.sum(exp_terms, axis=1)
    target_hit = col_ids[None, :] == targets[:, None].astype(jnp.int32)
    target_logit = jnp.sum(jnp.where(target_hit, capped, jnp.float32(0.0)), axis=1)
    token_loss = jnp.log(sums) - target_logit
    onehot = jnp.where(target_hit, jnp.float32(1.0), jnp.float32(0.0))
    logit_grad = (token_weight[:, None] * (exp_terms / sums[:, None] - onehot) * (1.0 - squash * squash)).astype(jnp.bfloat16)
    hidden_grad = jnp.dot(logit_grad, out_weight.T, preferred_element_type=jnp.float32).astype(jnp.bfloat16)
    hidden_blocks = hidden.reshape(N_DP, TOK_DEV, D)
    grad_blocks = logit_grad.reshape(N_DP, TOK_DEV, padded)

    def add_block(carried, pair):
        block_term = jnp.dot(pair[0].T, pair[1], preferred_element_type=jnp.float32).astype(jnp.bfloat16)
        block_term = lax.optimization_barrier(block_term)
        return carried + block_term.astype(jnp.float32), None

    summed, _ = lax.scan(add_block, jnp.zeros((D, padded), jnp.float32), (hidden_blocks, grad_blocks))
    return token_loss, hidden_grad, summed.astype(jnp.bfloat16)
```

```python
import functools

import jax
import jax.numpy as jnp
from jax import lax
from jax.experimental import pallas as pl
from jax.experimental.pallas import tpu as pltpu
from jax.sharding import PartitionSpec as P

softcap = 30.0
MESH = pl.DeviceIdType.MESH
NT = (((1,), (1,)), ((), ()))
TN = (((0,), (0,)), ((), ()))


def kernel(
    nv, nz, vocab_used,
    hidden, weight, targets, token_weight,
    loss_out, hg_out, wg_out,
    w, h, part, part_in, expo, slope, stat, lg, g_send, g_keep, r1, s2, r2, s3, r3, zb, hg, wg,
    loc_sem, snd_sem, rcv_sem,
):
    tok, rows = h.shape[1], h.shape[2]
    width = w.shape[1]
    half_tok = tok // 2
    grp = tok // nz
    cols = rows // 2
    x = lax.axis_index("dp")
    v = lax.axis_index("vocab")
    z, y, core = v // 4, (v // 2) % 2, v % 2
    ox, oy, oc = 1 - x, 1 - y, 1 - core

    def vid(zz, yy, cc):
        return zz * 4 + yy * 2 + cc

    peer_x = (ox, v)
    peer_c = (x, vid(z, y, oc))
    peer_y = (x, vid(z, oy, core))
    diag = (ox, vid(z, oy, core))

    def remote(src, dst, sem, dev, rsem=None):
        return pltpu.make_async_remote_copy(
            src_ref=src, dst_ref=dst, send_sem=snd_sem.at[sem],
            recv_sem=rcv_sem.at[sem if rsem is None else rsem],
            device_id=dev, device_id_type=MESH,
        )

    A_X, A_C, B0, LG, C0 = 0, 1, 2, 4, 5
    R1 = C0 + nv
    R2 = R1 + 2 * nz
    R3 = R2 + nz
    Z0 = R3 + nz
    X0 = Z0 + nz
    D0 = X0 + 2 * nz
    K0 = D0 + 2 * nz

    own_cols = pl.ds(pl.multiple_of(x * rows, 128), rows)
    oth_cols = pl.ds(pl.multiple_of(ox * rows, 128), rows)
    ld_h = pltpu.make_async_copy(hidden.at[:, own_cols], h.at[0], loc_sem.at[0])
    ld_w = pltpu.make_async_copy(weight, w, loc_sem.at[1])
    ld_h.start()
    ld_w.start()

    barrier = pltpu.get_barrier_semaphore()
    pl.semaphore_signal(barrier, inc=1, device_id=peer_x, device_id_type=MESH)
    pl.semaphore_signal(barrier, inc=1, device_id=diag, device_id_type=MESH)
    for j in range(1, nv):
        pl.semaphore_signal(barrier, inc=1, device_id=(x, (v + j) % nv), device_id_type=MESH)
    pl.semaphore_wait(barrier, nv + 1)

    def tok_half(c):
        return pl.ds(pl.multiple_of(c * half_tok, 16), half_tok)

    a_x = remote(hidden.at[tok_half(core), oth_cols], h.at[1, tok_half(core)], A_X, peer_x)
    a_x.start()

    ld_h.wait()
    ld_w.wait()
    part[2] = jnp.dot(h[0, :half_tok], w[...], preferred_element_type=jnp.float32)
    part[3] = jnp.dot(h[0, half_tok:], w[...], preferred_element_type=jnp.float32)
    a_x.wait_recv()
    a_c = remote(h.at[1, tok_half(core)], h.at[1, tok_half(core)], A_C, peer_c)
    a_c.start()
    sends = [a_x, a_c]
    part[core] = jnp.dot(h[1, tok_half(core)], w[...], preferred_element_type=jnp.float32)
    b0 = remote(part.at[core], part_in.at[core], B0, peer_x)
    b0.start()
    remote(h.at[1, tok_half(oc)], h.at[1, tok_half(oc)], A_C, peer_c).wait_recv()
    part[oc] = jnp.dot(h[1, tok_half(oc)], w[...], preferred_element_type=jnp.float32)
    b1 = remote(part.at[oc], part_in.at[oc], B0 + 1, peer_x)
    b1.start()
    sends += [b0, b1]
    b0.wait_recv()
    b1.wait_recv()

    col_ids = v * width + lax.broadcasted_iota(jnp.int32, (half_tok, width), 1)
    lane = lax.broadcasted_iota(jnp.int32, (half_tok, 128), 1)
    stats = []
    for i in range(2):
        sl = slice(i * half_tok, (i + 1) * half_tok)
        squash = jnp.tanh((part[2 + i] + part_in[i]) / softcap)
        capped = softcap * squash
        e = jnp.where(col_ids < vocab_used, jnp.exp(capped), 0.0)
        hit = col_ids == targets[sl]
        expo[sl] = e
        slope[sl] = 1.0 - squash * squash
        s_col = jnp.sum(e, axis=1, keepdims=True)
        t_col = jnp.sum(jnp.where(hit, capped, 0.0), axis=1, keepdims=True)
        stats.append(jnp.where(lane == 0, s_col, jnp.where(lane == 1, t_col, 0.0)))
    pad = jnp.zeros((stat.shape[2] - tok, 128), jnp.float32)
    stat[v] = jnp.concatenate(stats + [pad], axis=0).T[:8]
    for j in range(1, nv):
        c = remote(stat.at[v], stat.at[v], C0 + j, (x, (v + j) % nv))
        c.start()
        sends.append(c)
    for j in range(1, nv):
        src = (v + nv - j) % nv
        remote(stat.at[src], stat.at[src], C0 + j, (x, src)).wait_recv()
    total = stat[0]
    for i in range(1, nv):
        total = total + stat[i]
    loss_out[0:1] = jnp.log(total[0:1]) - total[1:2]
    wide = jnp.concatenate([total] + [jnp.zeros_like(total)] * 15, axis=0).T
    for i in range(2):
        sl = slice(i * half_tok, (i + 1) * half_tok)
        hit = col_ids == targets[sl]
        onehot = jnp.where(hit, jnp.float32(1.0), jnp.float32(0.0))
        lg[0, sl] = (
            token_weight[sl] * (expo[sl] / wide[sl, 0:1] - onehot) * slope[sl]
        ).astype(jnp.bfloat16)
    lg_x = remote(lg.at[0], lg.at[1], LG, peer_x)
    lg_x.start()
    sends.append(lg_x)

    step = cols // 3
    r1s = []
    for d in range(2):
        if d == 1:
            lg_x.wait_recv()
        tk = x if d == 0 else ox
        g = lg[d]
        for n in range(3):
            wr = w[pl.ds(pl.multiple_of(oc * cols + n * step, 16), step)]
            o = lax.dot_general(g, wr, NT, preferred_element_type=jnp.float32)
            for k in range(nz):
                g_send[tk, k, :, n * step:(n + 1) * step] = o[k * grp:(k + 1) * grp].astype(jnp.bfloat16)
        for k in range(nz):
            c = remote(g_send.at[tk, k], r1.at[tk, k], R1 + d * nz + k, peer_c)
            c.start()
            r1s.append(c)
        for n in range(3):
            wr = w[pl.ds(pl.multiple_of(core * cols + n * step, 16), step)]
            o = lax.dot_general(g, wr, NT, preferred_element_type=jnp.float32)
            for k in range(nz):
                g_keep[tk, k, :, n * step:(n + 1) * step] = o[k * grp:(k + 1) * grp]
    sends += r1s
    for c in r1s:
        c.wait_recv()

    r2s = []
    for j in range(nz):
        k = (z + 1 + j) % nz
        s2[k] = (g_keep[oy, k] + r1[oy, k].astype(jnp.float32)).astype(jnp.bfloat16)
        c = remote(s2.at[k], r2.at[k], R2 + j, peer_y)
        c.start()
        r2s.append(c)
    sends += r2s

    wstep = rows // 6
    for n in range(6):
        cs = slice(n * wstep, (n + 1) * wstep)
        o0 = lax.dot_general(h[0, :, cs], lg[0], TN, preferred_element_type=jnp.float32)
        o1 = lax.dot_general(h[1, :, cs], lg[1], TN, preferred_element_type=jnp.float32)
        o0 = o0.astype(jnp.bfloat16).astype(jnp.float32)
        o1 = o1.astype(jnp.bfloat16).astype(jnp.float32)
        wg[cs] = (o0 + o1).astype(jnp.bfloat16)
    st_w = pltpu.make_async_copy(wg, wg_out, loc_sem.at[2])
    st_w.start()

    r3s = []
    for j in range(nz):
        k = (z + 1 + j) % nz
        r2s[j].wait_recv()
        t = g_keep[y, k] + r1[y, k].astype(jnp.float32) + r2[k].astype(jnp.float32)
        if j < nz - 1:
            s3[k] = t.astype(jnp.bfloat16)
            c = remote(s3.at[k], r3.at[j], R3 + j, (x, vid(k, y, core)))
            c.start()
            r3s.append(c)
        else:
            mine = t
    sends += r3s
    for j in range(nz - 1):
        r3s[j].wait_recv()
        mine = mine + r3[j].astype(jnp.float32)
    zb[z] = mine.astype(jnp.bfloat16)

    zs = []
    for j in range(nz - 1):
        k = (z + 1 + j) % nz
        c = remote(zb.at[z], zb.at[z], Z0 + j, (x, vid(k, y, core)))
        c.start()
        zs.append(c)
    sends += zs

    def fan(k, j):
        @pl.when(x == y)
        def _():
            hg[x, core, k] = zb[k]
            remote(zb.at[k], hg.at[x, core, k], D0 + j, peer_y, X0 + nz + j).start()

        @pl.when(x != y)
        def _():
            remote(zb.at[k], hg.at[x, core, k], X0 + j, peer_x, X0 + j).start()
            remote(zb.at[k], hg.at[x, core, k], D0 + j, diag, D0 + j).start()

    for j in range(nz):
        src = (z + nz - j) % nz
        if j:
            remote(zb.at[src], zb.at[src], Z0 + j - 1, (x, vid(src, y, core))).wait_recv()
        fan(src, j)

    ks = []
    for j in range(nz):
        k = (z + nz - j) % nz

        @pl.when(x == y)
        def _():
            remote(hg.at[ox, core, k], hg.at[ox, core, k], X0 + j, peer_x).wait_recv()

        @pl.when(x != y)
        def _():
            remote(hg.at[x, core, k], hg.at[x, core, k], X0 + nz + j, peer_y).wait_recv()
            remote(hg.at[ox, core, k], hg.at[ox, core, k], D0 + j, diag).wait_recv()

        for xs in range(2):
            c = remote(hg.at[xs, core, k], hg.at[xs, core, k], K0 + 2 * j + xs, peer_c)
            c.start()
            ks.append(c)
    sends += ks
    for j in range(nz):
        k = (z + nz - j) % nz
        for xs in range(2):
            remote(hg.at[xs, oc, k], hg.at[xs, oc, k], K0 + 2 * j + xs, peer_c).wait_recv()
    st_h = pltpu.make_async_copy(hg, hg_out, loc_sem.at[3])
    st_h.start()

    for c in sends:
        c.wait_send()
    for j in range(nz):
        k = (z + nz - j) % nz

        @pl.when(x == y)
        def _():
            remote(zb.at[k], hg.at[x, core, k], D0 + j, peer_y).wait_send()

        @pl.when(x != y)
        def _():
            remote(zb.at[k], hg.at[x, core, k], X0 + j, peer_x).wait_send()
            remote(zb.at[k], hg.at[x, core, k], D0 + j, diag).wait_send()

    st_w.wait()
    st_h.wait()


def fused_body(hidden, out_weight, targets, token_weight):
    nv = lax.axis_size("vocab")
    nz = nv // 4
    tok = hidden.shape[0]
    rows, width = out_weight.shape
    grp, cols = tok // nz, rows // 2
    lanes = -(-tok // 128) * 128
    bf, f32 = jnp.bfloat16, jnp.float32
    anyspec = pl.BlockSpec(memory_space=pl.ANY)
    vspec = pl.BlockSpec(memory_space=pltpu.VMEM)
    nsem = 5 + nv + 11 * nz + nz
    loss, hg, wg = pl.pallas_call(
        functools.partial(kernel, nv, nz, width * nv - width // 2),
        out_shape=(
            jax.ShapeDtypeStruct((8, lanes), f32),
            jax.ShapeDtypeStruct((2, 2, nz, grp, cols), bf),
            jax.ShapeDtypeStruct((rows, width), bf),
        ),
        in_specs=[anyspec, anyspec, vspec, vspec],
        out_specs=(vspec, anyspec, anyspec),
        scratch_shapes=[
            pltpu.VMEM((rows, width), bf),
            pltpu.VMEM((2, tok, rows), bf),
            pltpu.VMEM((4, tok // 2, width), f32),
            pltpu.VMEM((2, tok // 2, width), f32),
            pltpu.VMEM((tok, width), f32),
            pltpu.VMEM((tok, width), f32),
            pltpu.VMEM((nv, 8, lanes), f32),
            pltpu.VMEM((2, tok, width), bf),
            pltpu.VMEM((2, nz, grp, cols), bf),
            pltpu.VMEM((2, nz, grp, cols), f32),
            pltpu.VMEM((2, nz, grp, cols), bf),
            pltpu.VMEM((nz, grp, cols), bf),
            pltpu.VMEM((nz, grp, cols), bf),
            pltpu.VMEM((nz, grp, cols), bf),
            pltpu.VMEM((nz, grp, cols), bf),
            pltpu.VMEM((nz, grp, cols), bf),
            pltpu.VMEM((2, 2, nz, grp, cols), bf),
            pltpu.VMEM((rows, width), bf),
            pltpu.SemaphoreType.DMA((4,)),
            pltpu.SemaphoreType.DMA((nsem,)),
            pltpu.SemaphoreType.DMA((nsem,)),
        ],
        compiler_params=pltpu.CompilerParams(
            collective_id=0, has_side_effects=True, vmem_limit_bytes=56 * 1024 * 1024
        ),
    )(hidden, out_weight, targets.reshape(tok, 1), token_weight.reshape(tok, 1))
    hidden_grad = hg.transpose(2, 3, 0, 1, 4).reshape(tok, 4 * cols)
    return loss[0, :tok], hidden_grad, wg


def plain_body(hidden, out_weight, targets, token_weight):
    shard_width = out_weight.shape[1]
    row_count = out_weight.shape[0]
    tok_rows = hidden.shape[0]
    vocab_used = shard_width * lax.axis_size("vocab") - shard_width // 2
    first_col = lax.axis_index("vocab") * shard_width
    col_ids = first_col + jnp.arange(shard_width, dtype=jnp.int32)
    usable = col_ids < vocab_used
    w_full = lax.all_gather(out_weight, "dp", axis=0, tiled=True)
    logits = jnp.dot(hidden, w_full, preferred_element_type=jnp.float32)
    squash = jnp.tanh(logits / softcap)
    capped = softcap * squash
    exp_terms = jnp.where(usable[None, :], jnp.exp(capped), jnp.float32(0.0))
    target_hit = col_ids[None, :] == targets[:, None]
    local_sum = jnp.sum(exp_terms, axis=1)
    local_target = jnp.sum(jnp.where(target_hit, capped, jnp.float32(0.0)), axis=1)
    sums, target_logit = lax.psum((local_sum, local_target), "vocab")
    token_loss = jnp.log(sums) - target_logit
    onehot = jnp.where(target_hit, jnp.float32(1.0), jnp.float32(0.0))
    logit_grad = (
        token_weight[:, None] * (exp_terms / sums[:, None] - onehot) * (1.0 - squash * squash)
    ).astype(jnp.bfloat16)
    partial_grad = lax.dot_general(logit_grad, w_full, NT, preferred_element_type=jnp.float32)
    share = lax.psum_scatter(partial_grad, "vocab", scatter_dimension=1, tiled=True).astype(
        jnp.bfloat16
    )
    hidden_grad = lax.all_gather(share, "vocab", axis=1, tiled=True)
    owned_cols = lax.all_to_all(hidden, "dp", split_axis=1, concat_axis=0, tiled=True)
    every_grad = lax.all_gather(logit_grad, "dp", axis=0, tiled=True)
    block_count = owned_cols.shape[0] // tok_rows
    col_blocks = owned_cols.reshape(block_count, tok_rows, row_count)
    grad_blocks = every_grad.reshape(block_count, tok_rows, shard_width)
    block_terms = jnp.einsum(
        "ntr,ntv->nrv", col_blocks, grad_blocks, preferred_element_type=jnp.float32
    ).astype(jnp.bfloat16)
    weight_grad = jnp.sum(block_terms.astype(jnp.float32), axis=0).astype(jnp.bfloat16)
    return (token_loss, hidden_grad, weight_grad)


def body(hidden, out_weight, targets, token_weight):
    nv = lax.axis_size("vocab")
    nz = nv // 4
    tok = hidden.shape[0]
    rows, width = out_weight.shape
    fits = (
        lax.axis_size("dp") == 2 and nv % 4 == 0 and tok % 32 == 0 and tok % (8 * nz) == 0
        and rows % 768 == 0 and width % 128 == 0
    )
    run = fused_body if fits else plain_body
    return run(hidden, out_weight, targets, token_weight)


def solution(mesh):
    placed = (P("dp", None), P("dp", "vocab"), P("dp"), P("dp"))
    return jax.shard_map(
        body,
        mesh=mesh,
        in_specs=placed,
        out_specs=(P("dp"), P("dp", None), P("dp", "vocab")),
        check_vma=False,
    )
```

```python
import functools

import jax
import jax.numpy as jnp
from jax import lax
from jax.experimental import pallas as pl
from jax.experimental.pallas import tpu as pltpu
from jax.sharding import PartitionSpec as P

softcap = 30.0
MESH = pl.DeviceIdType.MESH
NT = (((1,), (1,)), ((), ()))
TN = (((0,), (0,)), ((), ()))


def kernel(
    nv, nz, vocab_used,
    hidden, weight, targets, token_weight,
    loss_out, hg_out, wg_out,
    w, h, part, part_in, expo, slope, stat, lg, g_send, g_keep, r1, s2, r2, s3, r3, mine, zb, hg, wg,
    loc_sem, snd_sem, rcv_sem,
):
    tok, rows = h.shape[1], h.shape[2]
    width = w.shape[1]
    half_tok = tok // 2
    grp = tok // nz
    cols = rows // 2
    x = lax.axis_index("dp")
    v = lax.axis_index("vocab")
    z, y, core = v // 4, (v // 2) % 2, v % 2
    ox, oy, oc = 1 - x, 1 - y, 1 - core

    def vid(zz, yy, cc):
        return zz * 4 + yy * 2 + cc

    peer_x = (ox, v)
    peer_c = (x, vid(z, y, oc))
    peer_y = (x, vid(z, oy, core))
    diag = (ox, vid(z, oy, core))

    def remote(src, dst, sem, dev, rsem=None):
        return pltpu.make_async_remote_copy(
            src_ref=src, dst_ref=dst, send_sem=snd_sem.at[sem],
            recv_sem=rcv_sem.at[sem if rsem is None else rsem],
            device_id=dev, device_id_type=MESH,
        )

    A_X, A_C, B0, LG, C0 = 0, 1, 2, 4, 5
    R1 = C0 + nv
    R2 = R1 + 2 * nz
    R3 = R2 + 2 * nz
    Z0 = R3 + 2 * nz
    X0 = Z0 + 2 * nz
    Y0 = X0 + 2 * nz
    D0 = Y0 + 2 * nz
    K0 = D0 + 2 * nz

    first = -(-(cols // 128) // 2) * 128
    parts = [pl.ds(0, first), pl.ds(first, cols - first)]

    own_cols = pl.ds(pl.multiple_of(x * rows, 128), rows)
    oth_cols = pl.ds(pl.multiple_of(ox * rows, 128), rows)
    ld_h = pltpu.make_async_copy(hidden.at[:, own_cols], h.at[0], loc_sem.at[0])
    ld_w = pltpu.make_async_copy(weight, w, loc_sem.at[1])
    ld_h.start()
    ld_w.start()

    barrier = pltpu.get_barrier_semaphore()
    pl.semaphore_signal(barrier, inc=1, device_id=peer_x, device_id_type=MESH)
    pl.semaphore_signal(barrier, inc=1, device_id=diag, device_id_type=MESH)
    for j in range(1, nv):
        pl.semaphore_signal(barrier, inc=1, device_id=(x, (v + j) % nv), device_id_type=MESH)
    pl.semaphore_wait(barrier, nv + 1)

    def tok_half(c):
        return pl.ds(pl.multiple_of(c * half_tok, 16), half_tok)

    a_x = remote(hidden.at[tok_half(core), oth_cols], h.at[1, tok_half(core)], A_X, peer_x)
    a_x.start()

    ld_h.wait()
    ld_w.wait()
    part[2] = jnp.dot(h[0, :half_tok], w[...], preferred_element_type=jnp.float32)
    part[3] = jnp.dot(h[0, half_tok:], w[...], preferred_element_type=jnp.float32)
    a_x.wait_recv()
    a_c = remote(h.at[1, tok_half(core)], h.at[1, tok_half(core)], A_C, peer_c)
    a_c.start()
    sends = [a_x, a_c]
    part[core] = jnp.dot(h[1, tok_half(core)], w[...], preferred_element_type=jnp.float32)
    b0 = remote(part.at[core], part_in.at[core], B0, peer_x)
    b0.start()
    remote(h.at[1, tok_half(oc)], h.at[1, tok_half(oc)], A_C, peer_c).wait_recv()
    part[oc] = jnp.dot(h[1, tok_half(oc)], w[...], preferred_element_type=jnp.float32)
    b1 = remote(part.at[oc], part_in.at[oc], B0 + 1, peer_x)
    b1.start()
    sends += [b0, b1]
    b0.wait_recv()
    b1.wait_recv()

    def column(ref):
        row = ref[...].reshape(1, tok)
        row = jnp.concatenate([row, jnp.zeros((1, stat.shape[2] - tok), row.dtype)], axis=1)
        return jnp.broadcast_to(row, (128, stat.shape[2])).T[:tok, 0:1]

    target_col, weight_col = column(targets), column(token_weight)
    col_ids = v * width + lax.broadcasted_iota(jnp.int32, (half_tok, width), 1)
    lane = lax.broadcasted_iota(jnp.int32, (half_tok, 128), 1)
    stats = []
    for i in range(2):
        sl = slice(i * half_tok, (i + 1) * half_tok)
        squash = jnp.tanh((part[2 + i] + part_in[i]) / softcap)
        capped = softcap * squash
        e = jnp.where(col_ids < vocab_used, jnp.exp(capped), 0.0)
        hit = col_ids == target_col[sl]
        expo[sl] = e
        slope[sl] = 1.0 - squash * squash
        s_col = jnp.sum(e, axis=1, keepdims=True)
        t_col = jnp.sum(jnp.where(hit, capped, 0.0), axis=1, keepdims=True)
        stats.append(jnp.where(lane == 0, s_col, jnp.where(lane == 1, t_col, 0.0)))
    pad = jnp.zeros((stat.shape[2] - tok, 128), jnp.float32)
    stat[v] = jnp.concatenate(stats + [pad], axis=0).T[:8]
    for j in range(1, nv):
        c = remote(stat.at[v], stat.at[v], C0 + j, (x, (v + j) % nv))
        c.start()
        sends.append(c)
    for j in range(1, nv):
        src = (v + nv - j) % nv
        remote(stat.at[src], stat.at[src], C0 + j, (x, src)).wait_recv()
    total = stat[0]
    for i in range(1, nv):
        total = total + stat[i]
    loss_out[...] = (jnp.log(total[0:1]) - total[1:2])[:, :tok].reshape(tok)
    wide = jnp.concatenate([total] + [jnp.zeros_like(total)] * 15, axis=0).T
    for i in range(2):
        sl = slice(i * half_tok, (i + 1) * half_tok)
        hit = col_ids == target_col[sl]
        onehot = jnp.where(hit, jnp.float32(1.0), jnp.float32(0.0))
        lg[0, sl] = (
            weight_col[sl] * (expo[sl] / wide[sl, 0:1] - onehot) * slope[sl]
        ).astype(jnp.bfloat16)
    lg_x = remote(lg.at[0], lg.at[1], LG, peer_x)
    lg_x.start()
    sends.append(lg_x)

    step = cols // 3
    r1s = []
    for d in range(2):
        if d == 1:
            lg_x.wait_recv()
        tk = x if d == 0 else ox
        g = lg[d]
        for n in range(3):
            wr = w[pl.ds(pl.multiple_of(oc * cols + n * step, 16), step)]
            o = lax.dot_general(g, wr, NT, preferred_element_type=jnp.float32)
            for k in range(nz):
                g_send[tk, k, :, n * step:(n + 1) * step] = o[k * grp:(k + 1) * grp].astype(jnp.bfloat16)
        for k in range(nz):
            c = remote(g_send.at[tk, k], r1.at[tk, k], R1 + tk * nz + k, peer_c)
            c.start()
            r1s.append(c)
        for n in range(3):
            wr = w[pl.ds(pl.multiple_of(core * cols + n * step, 16), step)]
            o = lax.dot_general(g, wr, NT, preferred_element_type=jnp.float32)
            for k in range(nz):
                g_keep[tk, k, :, n * step:(n + 1) * step] = o[k * grp:(k + 1) * grp]
    sends += r1s

    def from_partner(d, k):
        remote(r1.at[d, k], r1.at[d, k], R1 + d * nz + k, peer_c).wait_recv()

    r2s = []
    for p, cs in enumerate(parts):
        for j in range(nz):
            k = (z + 1 + j) % nz
            if p == 0:
                from_partner(oy, k)
            s2[k, :, cs] = (g_keep[oy, k, :, cs] + r1[oy, k, :, cs].astype(jnp.float32)).astype(
                jnp.bfloat16
            )
            c = remote(s2.at[k, :, cs], r2.at[k, :, cs], R2 + p * nz + j, peer_y)
            c.start()
            r2s.append(c)
    sends += r2s

    wstep = rows // 6

    def weight_part(n):
        cs = slice(n * wstep, (n + 1) * wstep)
        o0 = lax.dot_general(h[0, :, cs], lg[0], TN, preferred_element_type=jnp.float32)
        o1 = lax.dot_general(h[1, :, cs], lg[1], TN, preferred_element_type=jnp.float32)
        o0 = o0.astype(jnp.bfloat16).astype(jnp.float32)
        o1 = o1.astype(jnp.bfloat16).astype(jnp.float32)
        wg[cs] = (o0 + o1).astype(jnp.bfloat16)

    r3s = []
    for p, cs in enumerate(parts):
        for j in range(nz):
            k = (z + 1 + j) % nz
            if p == 0:
                from_partner(y, k)
            r2s[p * nz + j].wait_recv()
            t = (
                g_keep[y, k, :, cs]
                + r1[y, k, :, cs].astype(jnp.float32)
                + r2[k, :, cs].astype(jnp.float32)
            )
            if j < nz - 1:
                s3[k, :, cs] = t.astype(jnp.bfloat16)
                c = remote(
                    s3.at[k, :, cs], r3.at[j, :, cs], R3 + p * nz + j, (x, vid(k, y, core))
                )
                c.start()
                r3s.append(c)
            else:
                mine[:, cs] = t
        if p == 0:
            for n in range(3):
                weight_part(n)
    sends += r3s

    zs = []
    for p, cs in enumerate(parts):
        t = mine[:, cs]
        for j in range(nz - 1):
            r3s[p * (nz - 1) + j].wait_recv()
            t = t + r3[j, :, cs].astype(jnp.float32)
        zb[z, :, cs] = t.astype(jnp.bfloat16)
        for j in range(nz - 1):
            k = (z + 1 + j) % nz
            c = remote(zb.at[z, :, cs], zb.at[z, :, cs], Z0 + p * nz + j, (x, vid(k, y, core)))
            c.start()
            zs.append(c)
        if p == 0:
            for n in range(3, 6):
                weight_part(n)
            st_w = pltpu.make_async_copy(wg, wg_out, loc_sem.at[2])
            st_w.start()
    sends += zs

    def fan(p, k, j):
        cs, i = parts[p], p * nz + j
        src, dst = zb.at[k, :, cs], hg.at[x, core, k, :, cs]
        return (
            remote(src, dst, D0 + i, peer_y, Y0 + i),
            remote(src, dst, X0 + i, peer_x, X0 + i),
            remote(src, dst, D0 + i, diag, D0 + i),
        )

    for p, cs in enumerate(parts):
        for j in range(nz):
            k = (z + nz - j) % nz
            if j:
                remote(
                    zb.at[k, :, cs], zb.at[k, :, cs], Z0 + p * nz + j - 1, (x, vid(k, y, core))
                ).wait_recv()
            to_y, to_x, to_diag = fan(p, k, j)

            @pl.when(x == y)
            def _():
                to_y.start()
                hg[x, core, k, :, cs] = zb[k, :, cs]

            @pl.when(x != y)
            def _():
                to_x.start()
                to_diag.start()

    ks = []
    for p, cs in enumerate(parts):
        for j in range(nz):
            k = (z + nz - j) % nz
            i = p * nz + j

            @pl.when(x == y)
            def _():
                remote(hg.at[ox, core, k, :, cs], hg.at[ox, core, k, :, cs], X0 + i, peer_x).wait_recv()

            @pl.when(x != y)
            def _():
                remote(hg.at[x, core, k, :, cs], hg.at[x, core, k, :, cs], Y0 + i, peer_y).wait_recv()
                remote(hg.at[ox, core, k, :, cs], hg.at[ox, core, k, :, cs], D0 + i, diag).wait_recv()

            for xs in range(2):
                spot = hg.at[xs, core, k, :, cs]
                c = remote(spot, spot, K0 + 2 * i + xs, peer_c)
                c.start()
                ks.append(c)
    sends += ks

    outs = []

    def put(cc, xs, k, n):
        c = pltpu.make_async_copy(
            hg.at[xs, cc, k],
            hg_out.at[
                pl.ds(pl.multiple_of(k * grp, 8), grp),
                pl.ds(pl.multiple_of(xs * rows + cc * cols, 128), cols),
            ],
            loc_sem.at[3 + n],
        )
        c.start()
        outs.append(c)

    for j in range(nz):
        k = (z + nz - j) % nz
        for xs in range(2):
            put(core, xs, k, 4 * j + xs)
    for j in range(nz):
        k = (z + nz - j) % nz
        for xs in range(2):
            for p, cs in enumerate(parts):
                spot = hg.at[xs, oc, k, :, cs]
                remote(spot, spot, K0 + 2 * (p * nz + j) + xs, peer_c).wait_recv()
            put(oc, xs, k, 4 * j + 2 + xs)

    for c in sends:
        c.wait_send()
    for p in range(2):
        for j in range(nz):
            to_y, to_x, to_diag = fan(p, (z + nz - j) % nz, j)

            @pl.when(x == y)
            def _():
                to_y.wait_send()

            @pl.when(x != y)
            def _():
                to_x.wait_send()
                to_diag.wait_send()

    st_w.wait()
    for c in outs:
        c.wait()


def fused_body(hidden, out_weight, targets, token_weight):
    nv = lax.axis_size("vocab")
    nz = nv // 4
    tok = hidden.shape[0]
    rows, width = out_weight.shape
    grp, cols = tok // nz, rows // 2
    lanes = -(-tok // 128) * 128
    bf, f32 = jnp.bfloat16, jnp.float32
    anyspec = pl.BlockSpec(memory_space=pl.ANY)
    vspec = pl.BlockSpec(memory_space=pltpu.VMEM)
    nsem = 5 + nv + 20 * nz
    loss, hg, wg = pl.pallas_call(
        functools.partial(kernel, nv, nz, width * nv - width // 2),
        out_shape=(
            jax.ShapeDtypeStruct((tok,), f32),
            jax.ShapeDtypeStruct((tok, 2 * rows), bf),
            jax.ShapeDtypeStruct((rows, width), bf),
        ),
        in_specs=[anyspec, anyspec, vspec, vspec],
        out_specs=(vspec, anyspec, anyspec),
        scratch_shapes=[
            pltpu.VMEM((rows, width), bf),
            pltpu.VMEM((2, tok, rows), bf),
            pltpu.VMEM((4, tok // 2, width), f32),
            pltpu.VMEM((2, tok // 2, width), f32),
            pltpu.VMEM((tok, width), f32),
            pltpu.VMEM((tok, width), f32),
            pltpu.VMEM((nv, 8, lanes), f32),
            pltpu.VMEM((2, tok, width), bf),
            pltpu.VMEM((2, nz, grp, cols), bf),
            pltpu.VMEM((2, nz, grp, cols), f32),
            pltpu.VMEM((2, nz, grp, cols), bf),
            pltpu.VMEM((nz, grp, cols), bf),
            pltpu.VMEM((nz, grp, cols), bf),
            pltpu.VMEM((nz, grp, cols), bf),
            pltpu.VMEM((nz, grp, cols), bf),
            pltpu.VMEM((grp, cols), f32),
            pltpu.VMEM((nz, grp, cols), bf),
            pltpu.VMEM((2, 2, nz, grp, cols), bf),
            pltpu.VMEM((rows, width), bf),
            pltpu.SemaphoreType.DMA((3 + 4 * nz,)),
            pltpu.SemaphoreType.DMA((nsem,)),
            pltpu.SemaphoreType.DMA((nsem,)),
        ],
        compiler_params=pltpu.CompilerParams(
            collective_id=0, has_side_effects=True, vmem_limit_bytes=56 * 1024 * 1024
        ),
    )(hidden, out_weight, targets, token_weight)
    return loss, hg, wg


def plain_body(hidden, out_weight, targets, token_weight):
    shard_width = out_weight.shape[1]
    row_count = out_weight.shape[0]
    tok_rows = hidden.shape[0]
    vocab_used = shard_width * lax.axis_size("vocab") - shard_width // 2
    first_col = lax.axis_index("vocab") * shard_width
    col_ids = first_col + jnp.arange(shard_width, dtype=jnp.int32)
    usable = col_ids < vocab_used
    w_full = lax.all_gather(out_weight, "dp", axis=0, tiled=True)
    logits = jnp.dot(hidden, w_full, preferred_element_type=jnp.float32)
    squash = jnp.tanh(logits / softcap)
    capped = softcap * squash
    exp_terms = jnp.where(usable[None, :], jnp.exp(capped), jnp.float32(0.0))
    target_hit = col_ids[None, :] == targets[:, None]
    local_sum = jnp.sum(exp_terms, axis=1)
    local_target = jnp.sum(jnp.where(target_hit, capped, jnp.float32(0.0)), axis=1)
    sums, target_logit = lax.psum((local_sum, local_target), "vocab")
    token_loss = jnp.log(sums) - target_logit
    onehot = jnp.where(target_hit, jnp.float32(1.0), jnp.float32(0.0))
    logit_grad = (
        token_weight[:, None] * (exp_terms / sums[:, None] - onehot) * (1.0 - squash * squash)
    ).astype(jnp.bfloat16)
    partial_grad = lax.dot_general(logit_grad, w_full, NT, preferred_element_type=jnp.float32)
    share = lax.psum_scatter(partial_grad, "vocab", scatter_dimension=1, tiled=True).astype(
        jnp.bfloat16
    )
    hidden_grad = lax.all_gather(share, "vocab", axis=1, tiled=True)
    owned_cols = lax.all_to_all(hidden, "dp", split_axis=1, concat_axis=0, tiled=True)
    every_grad = lax.all_gather(logit_grad, "dp", axis=0, tiled=True)
    block_count = owned_cols.shape[0] // tok_rows
    col_blocks = owned_cols.reshape(block_count, tok_rows, row_count)
    grad_blocks = every_grad.reshape(block_count, tok_rows, shard_width)
    block_terms = jnp.einsum(
        "ntr,ntv->nrv", col_blocks, grad_blocks, preferred_element_type=jnp.float32
    ).astype(jnp.bfloat16)
    weight_grad = jnp.sum(block_terms.astype(jnp.float32), axis=0).astype(jnp.bfloat16)
    return (token_loss, hidden_grad, weight_grad)


def body(hidden, out_weight, targets, token_weight):
    nv = lax.axis_size("vocab")
    nz = nv // 4
    tok = hidden.shape[0]
    rows, width = out_weight.shape
    fits = (
        lax.axis_size("dp") == 2 and nv % 4 == 0 and tok % 32 == 0 and tok % (8 * nz) == 0
        and rows % 768 == 0 and width % 128 == 0
    )
    run = fused_body if fits else plain_body
    return run(hidden, out_weight, targets, token_weight)


def solution(mesh):
    placed = (P("dp", None), P("dp", "vocab"), P("dp"), P("dp"))
    return jax.shard_map(
        body,
        mesh=mesh,
        in_specs=placed,
        out_specs=(P("dp"), P("dp", None), P("dp", "vocab")),
        check_vma=False,
    )
```

```python
import functools

import jax
import jax.numpy as jnp
from jax import lax
from jax.experimental import pallas as pl
from jax.experimental.pallas import tpu as pltpu
from jax.sharding import PartitionSpec as P

softcap = 30.0
MESH = pl.DeviceIdType.MESH
NT = (((1,), (1,)), ((), ()))
TN = (((0,), (0,)), ((), ()))


def kernel(
    nv, nz, vocab_used,
    hidden, weight, targets, token_weight,
    loss_out, hg_out, wg_out,
    w, h, h1, part, part_out, part_in, expo, slope, stat, lg, g_send, g_keep, r1, s2, r2, s3, r3, mine, zb, relay, hg, wg,
    loc_sem, snd_sem, rcv_sem,
):
    tok, rows = h.shape[1], h.shape[2]
    width = w.shape[1]
    grp4 = tok // 4
    grp = tok // nz
    cols = rows // 2
    x = lax.axis_index("dp")
    v = lax.axis_index("vocab")
    z, y, core = v // 4, (v // 2) % 2, v % 2
    ox, oy, oc = 1 - x, 1 - y, 1 - core

    def vid(zz, yy, cc):
        return zz * 4 + yy * 2 + cc

    peer_x = (ox, v)
    peer_c = (x, vid(z, y, oc))
    peer_y = (x, vid(z, oy, core))

    def remote(src, dst, sem, dev, rsem=None):
        return pltpu.make_async_remote_copy(
            src_ref=src, dst_ref=dst, send_sem=snd_sem.at[sem],
            recv_sem=rcv_sem.at[sem if rsem is None else rsem],
            device_id=dev, device_id_type=MESH,
        )

    A_X, A_Y, A_C, A_CY, B0, LG, C0 = 0, 1, 2, 3, 4, 8, 9
    R1 = C0 + nv
    R2 = R1 + 2 * nz
    R3 = R2 + 2 * nz
    Z0 = R3 + 2 * nz
    X0 = Z0 + 2 * nz
    Y0 = X0 + 2 * nz
    K0 = Y0 + 2 * nz

    first = -(-(cols // 128) // 2) * 128
    parts = [pl.ds(0, first), pl.ds(first, cols - first)]

    own_cols = pl.ds(pl.multiple_of(x * rows, 128), rows)
    oth_cols = pl.ds(pl.multiple_of(ox * rows, 128), rows)
    ld_h = pltpu.make_async_copy(hidden.at[:, own_cols], h.at[0], loc_sem.at[0])
    ld_w = pltpu.make_async_copy(weight, w, loc_sem.at[1])
    ld_h.start()
    ld_w.start()

    barrier = pltpu.get_barrier_semaphore()
    pl.semaphore_signal(barrier, inc=1, device_id=peer_x, device_id_type=MESH)
    for j in range(1, nv):
        pl.semaphore_signal(barrier, inc=1, device_id=(x, (v + j) % nv), device_id_type=MESH)
    pl.semaphore_wait(barrier, nv)

    def piece(yy, cc):
        return h1.at[2 * yy + cc]

    q = 2 * y + core
    a_x = remote(
        hidden.at[pl.ds(pl.multiple_of(q * grp4, 8), grp4), oth_cols], piece(y, core), A_X, peer_x
    )
    a_x.start()
    ld_h.wait()
    ld_w.wait()
    part[...] = jnp.dot(h[0], w[...], preferred_element_type=jnp.float32)
    a_x.wait_recv()
    a_y = remote(piece(y, core), piece(y, core), A_Y, peer_y)
    a_y.start()
    a_c = remote(piece(y, core), piece(y, core), A_C, peer_c)
    a_c.start()
    sends = [a_x, a_y, a_c]
    bs = []

    def send_part(n, yy, cc):
        i = 2 * yy + cc
        part_out[i] = jnp.dot(h1[i], w[...], preferred_element_type=jnp.float32)
        c = remote(part_out.at[i], part_in.at[i], B0 + n, peer_x)
        c.start()
        bs.append(c)

    send_part(0, y, core)
    remote(piece(y, oc), piece(y, oc), A_C, peer_c).wait_recv()
    send_part(1, y, oc)
    remote(piece(oy, core), piece(oy, core), A_Y, peer_y).wait_recv()
    a_cy = remote(piece(oy, core), piece(oy, core), A_CY, peer_c)
    a_cy.start()
    sends.append(a_cy)
    send_part(2, oy, core)
    remote(piece(oy, oc), piece(oy, oc), A_CY, peer_c).wait_recv()
    send_part(3, oy, oc)
    sends += bs
    for c in bs:
        c.wait_recv()

    def column(ref):
        row = ref[...].reshape(1, tok)
        row = jnp.concatenate([row, jnp.zeros((1, stat.shape[2] - tok), row.dtype)], axis=1)
        return jnp.broadcast_to(row, (128, stat.shape[2])).T[:tok, 0:1]

    target_col, weight_col = column(targets), column(token_weight)
    col_ids = v * width + lax.broadcasted_iota(jnp.int32, (grp4, width), 1)
    lane = lax.broadcasted_iota(jnp.int32, (grp4, 128), 1)
    stats = []
    for i in range(4):
        sl = slice(i * grp4, (i + 1) * grp4)
        squash = jnp.tanh((part[sl] + part_in[i]) / softcap)
        capped = softcap * squash
        e = jnp.where(col_ids < vocab_used, jnp.exp(capped), 0.0)
        hit = col_ids == target_col[sl]
        expo[sl] = e
        slope[sl] = 1.0 - squash * squash
        s_col = jnp.sum(e, axis=1, keepdims=True)
        t_col = jnp.sum(jnp.where(hit, capped, 0.0), axis=1, keepdims=True)
        stats.append(jnp.where(lane == 0, s_col, jnp.where(lane == 1, t_col, 0.0)))
    pad = jnp.zeros((stat.shape[2] - tok, 128), jnp.float32)
    stat[v] = jnp.concatenate(stats + [pad], axis=0).T[:8]
    for j in range(1, nv):
        c = remote(stat.at[v], stat.at[v], C0 + j, (x, (v + j) % nv))
        c.start()
        sends.append(c)
    for j in range(1, nv):
        src = (v + nv - j) % nv
        remote(stat.at[src], stat.at[src], C0 + j, (x, src)).wait_recv()
    total = stat[0]
    for i in range(1, nv):
        total = total + stat[i]
    loss_out[...] = (jnp.log(total[0:1]) - total[1:2])[:, :tok].reshape(tok)
    grads = []
    wide = jnp.concatenate([total] + [jnp.zeros_like(total)] * 15, axis=0).T
    for i in range(4):
        sl = slice(i * grp4, (i + 1) * grp4)
        hit = col_ids == target_col[sl]
        onehot = jnp.where(hit, jnp.float32(1.0), jnp.float32(0.0))
        grads.append(weight_col[sl] * (expo[sl] / wide[sl, 0:1] - onehot) * slope[sl])
    lg[0] = jnp.concatenate(grads, axis=0).astype(jnp.bfloat16)
    lg_x = remote(lg.at[0], lg.at[1], LG, peer_x)
    lg_x.start()
    sends.append(lg_x)

    step = cols // 3
    r1s = []
    for d in range(2):
        if d == 1:
            lg_x.wait_recv()
        tk = x if d == 0 else ox
        g = lg[d]
        for n in range(3):
            wr = w[pl.ds(pl.multiple_of(oc * cols + n * step, 16), step)]
            o = lax.dot_general(g, wr, NT, preferred_element_type=jnp.float32)
            for k in range(nz):
                g_send[tk, k, :, n * step:(n + 1) * step] = o[k * grp:(k + 1) * grp].astype(jnp.bfloat16)
        for k in range(nz):
            c = remote(g_send.at[tk, k], r1.at[tk, k], R1 + tk * nz + k, peer_c)
            c.start()
            r1s.append(c)
        for n in range(3):
            wr = w[pl.ds(pl.multiple_of(core * cols + n * step, 16), step)]
            o = lax.dot_general(g, wr, NT, preferred_element_type=jnp.float32)
            for k in range(nz):
                g_keep[tk, k, :, n * step:(n + 1) * step] = o[k * grp:(k + 1) * grp]
    sends += r1s

    def from_partner(d, k):
        remote(r1.at[d, k], r1.at[d, k], R1 + d * nz + k, peer_c).wait_recv()

    r2s = []
    for p, cs in enumerate(parts):
        for j in range(nz):
            k = (z + 1 + j) % nz
            if p == 0:
                from_partner(oy, k)
            s2[k, :, cs] = (g_keep[oy, k, :, cs] + r1[oy, k, :, cs].astype(jnp.float32)).astype(
                jnp.bfloat16
            )
            c = remote(s2.at[k, :, cs], r2.at[k, :, cs], R2 + p * nz + j, peer_y)
            c.start()
            r2s.append(c)
    sends += r2s

    wstep = rows // 6
    for i in range(4):
        h[1, i * grp4:(i + 1) * grp4] = h1[i]

    def weight_part(n):
        cs = slice(n * wstep, (n + 1) * wstep)
        o0 = lax.dot_general(h[0, :, cs], lg[0], TN, preferred_element_type=jnp.float32)
        o1 = lax.dot_general(h[1, :, cs], lg[1], TN, preferred_element_type=jnp.float32)
        o0 = o0.astype(jnp.bfloat16).astype(jnp.float32)
        o1 = o1.astype(jnp.bfloat16).astype(jnp.float32)
        wg[cs] = (o0 + o1).astype(jnp.bfloat16)

    r3s = []
    for p, cs in enumerate(parts):
        for j in range(nz):
            k = (z + 1 + j) % nz
            if p == 0:
                from_partner(y, k)
            r2s[p * nz + j].wait_recv()
            t = (
                g_keep[y, k, :, cs]
                + r1[y, k, :, cs].astype(jnp.float32)
                + r2[k, :, cs].astype(jnp.float32)
            )
            if j < nz - 1:
                s3[k, :, cs] = t.astype(jnp.bfloat16)
                c = remote(
                    s3.at[k, :, cs], r3.at[j, :, cs], R3 + p * nz + j, (x, vid(k, y, core))
                )
                c.start()
                r3s.append(c)
            else:
                mine[:, cs] = t
        if p == 0:
            for n in range(3):
                weight_part(n)
    sends += r3s

    zs = []
    for p, cs in enumerate(parts):
        t = mine[:, cs]
        for j in range(nz - 1):
            r3s[p * (nz - 1) + j].wait_recv()
            t = t + r3[j, :, cs].astype(jnp.float32)
        zb[z, :, cs] = t.astype(jnp.bfloat16)
        for j in range(nz - 1):
            k = (z + 1 + j) % nz
            c = remote(zb.at[z, :, cs], zb.at[z, :, cs], Z0 + p * nz + j, (x, vid(k, y, core)))
            c.start()
            zs.append(c)
        if p == 0:
            for n in range(3, 6):
                weight_part(n)
            st_w = pltpu.make_async_copy(wg, wg_out, loc_sem.at[2])
            st_w.start()
    sends += zs

    def fan(p, k, j):
        cs, i = parts[p], p * nz + j
        src, dst = zb.at[k, :, cs], hg.at[x, core, k, :, cs]
        hop = relay.at[k, :, cs]
        return (
            remote(src, dst, Y0 + i, peer_y),
            remote(hop, dst, X0 + i, peer_x),
            remote(src, dst, X0 + i, peer_x),
            remote(src, hop, Y0 + i, peer_y),
        )

    def relay_on(p, k, j):
        @pl.when(x == y)
        def _():
            hop = relay.at[k, :, parts[p]]
            remote(hop, hop, Y0 + p * nz + j, peer_y).wait_recv()
            fan(p, k, j)[1].start()

    for p, cs in enumerate(parts):
        for j in range(nz):
            k = (z + nz - j) % nz
            if j:
                remote(
                    zb.at[k, :, cs], zb.at[k, :, cs], Z0 + p * nz + j - 1, (x, vid(k, y, core))
                ).wait_recv()
            home_y, home_x, away_x, away_y = fan(p, k, j)

            @pl.when(x == y)
            def _():
                home_y.start()
                hg[x, core, k, :, cs] = zb[k, :, cs]

            @pl.when(x != y)
            def _():
                away_y.start()
                away_x.start()

            if j or p:
                relay_on(*last)
            last = (p, k, j)
    relay_on(*last)

    ks = []
    for p, cs in enumerate(parts):
        for j in range(nz):
            k = (z + nz - j) % nz
            i = p * nz + j

            @pl.when(x != y)
            def _():
                spot = hg.at[x, core, k, :, cs]
                remote(spot, spot, Y0 + i, peer_y).wait_recv()

            spot = hg.at[ox, core, k, :, cs]
            remote(spot, spot, X0 + i, peer_x).wait_recv()

            for xs in range(2):
                spot = hg.at[xs, core, k, :, cs]
                c = remote(spot, spot, K0 + 2 * i + xs, peer_c)
                c.start()
                ks.append(c)
    sends += ks

    outs = []

    def put(cc, xs, k, n):
        c = pltpu.make_async_copy(
            hg.at[xs, cc, k],
            hg_out.at[
                pl.ds(pl.multiple_of(k * grp, 8), grp),
                pl.ds(pl.multiple_of(xs * rows + cc * cols, 128), cols),
            ],
            loc_sem.at[3 + n],
        )
        c.start()
        outs.append(c)

    for j in range(nz):
        k = (z + nz - j) % nz
        for xs in range(2):
            put(core, xs, k, 4 * j + xs)
    for j in range(nz):
        k = (z + nz - j) % nz
        for xs in range(2):
            for p, cs in enumerate(parts):
                spot = hg.at[xs, oc, k, :, cs]
                remote(spot, spot, K0 + 2 * (p * nz + j) + xs, peer_c).wait_recv()
            put(oc, xs, k, 4 * j + 2 + xs)

    for c in sends:
        c.wait_send()
    for p in range(2):
        for j in range(nz):
            home_y, home_x, away_x, away_y = fan(p, (z + nz - j) % nz, j)

            @pl.when(x == y)
            def _():
                home_y.wait_send()
                home_x.wait_send()

            @pl.when(x != y)
            def _():
                away_y.wait_send()
                away_x.wait_send()

    st_w.wait()
    for c in outs:
        c.wait()


def fused_body(hidden, out_weight, targets, token_weight):
    nv = lax.axis_size("vocab")
    nz = nv // 4
    tok = hidden.shape[0]
    rows, width = out_weight.shape
    grp, cols = tok // nz, rows // 2
    lanes = -(-tok // 128) * 128
    bf, f32 = jnp.bfloat16, jnp.float32
    anyspec = pl.BlockSpec(memory_space=pl.ANY)
    vspec = pl.BlockSpec(memory_space=pltpu.VMEM)
    nsem = 9 + nv + 16 * nz
    loss, hg, wg = pl.pallas_call(
        functools.partial(kernel, nv, nz, width * nv - width // 2),
        out_shape=(
            jax.ShapeDtypeStruct((tok,), f32),
            jax.ShapeDtypeStruct((tok, 2 * rows), bf),
            jax.ShapeDtypeStruct((rows, width), bf),
        ),
        in_specs=[anyspec, anyspec, vspec, vspec],
        out_specs=(vspec, anyspec, anyspec),
        scratch_shapes=[
            pltpu.VMEM((rows, width), bf),
            pltpu.VMEM((2, tok, rows), bf),
            pltpu.VMEM((4, tok // 4, rows), bf),
            pltpu.VMEM((tok, width), f32),
            pltpu.VMEM((4, tok // 4, width), f32),
            pltpu.VMEM((4, tok // 4, width), f32),
            pltpu.VMEM((tok, width), f32),
            pltpu.VMEM((tok, width), f32),
            pltpu.VMEM((nv, 8, lanes), f32),
            pltpu.VMEM((2, tok, width), bf),
            pltpu.VMEM((2, nz, grp, cols), bf),
            pltpu.VMEM((2, nz, grp, cols), f32),
            pltpu.VMEM((2, nz, grp, cols), bf),
            pltpu.VMEM((nz, grp, cols), bf),
            pltpu.VMEM((nz, grp, cols), bf),
            pltpu.VMEM((nz, grp, cols), bf),
            pltpu.VMEM((nz, grp, cols), bf),
            pltpu.VMEM((grp, cols), f32),
            pltpu.VMEM((nz, grp, cols), bf),
            pltpu.VMEM((nz, grp, cols), bf),
            pltpu.VMEM((2, 2, nz, grp, cols), bf),
            pltpu.VMEM((rows, width), bf),
            pltpu.SemaphoreType.DMA((3 + 4 * nz,)),
            pltpu.SemaphoreType.DMA((nsem,)),
            pltpu.SemaphoreType.DMA((nsem,)),
        ],
        compiler_params=pltpu.CompilerParams(
            collective_id=0, has_side_effects=True, vmem_limit_bytes=56 * 1024 * 1024
        ),
    )(hidden, out_weight, targets, token_weight)
    return loss, hg, wg


def plain_body(hidden, out_weight, targets, token_weight):
    shard_width = out_weight.shape[1]
    row_count = out_weight.shape[0]
    tok_rows = hidden.shape[0]
    vocab_used = shard_width * lax.axis_size("vocab") - shard_width // 2
    first_col = lax.axis_index("vocab") * shard_width
    col_ids = first_col + jnp.arange(shard_width, dtype=jnp.int32)
    usable = col_ids < vocab_used
    w_full = lax.all_gather(out_weight, "dp", axis=0, tiled=True)
    logits = jnp.dot(hidden, w_full, preferred_element_type=jnp.float32)
    squash = jnp.tanh(logits / softcap)
    capped = softcap * squash
    exp_terms = jnp.where(usable[None, :], jnp.exp(capped), jnp.float32(0.0))
    target_hit = col_ids[None, :] == targets[:, None]
    local_sum = jnp.sum(exp_terms, axis=1)
    local_target = jnp.sum(jnp.where(target_hit, capped, jnp.float32(0.0)), axis=1)
    sums, target_logit = lax.psum((local_sum, local_target), "vocab")
    token_loss = jnp.log(sums) - target_logit
    onehot = jnp.where(target_hit, jnp.float32(1.0), jnp.float32(0.0))
    logit_grad = (
        token_weight[:, None] * (exp_terms / sums[:, None] - onehot) * (1.0 - squash * squash)
    ).astype(jnp.bfloat16)
    partial_grad = lax.dot_general(logit_grad, w_full, NT, preferred_element_type=jnp.float32)
    share = lax.psum_scatter(partial_grad, "vocab", scatter_dimension=1, tiled=True).astype(
        jnp.bfloat16
    )
    hidden_grad = lax.all_gather(share, "vocab", axis=1, tiled=True)
    owned_cols = lax.all_to_all(hidden, "dp", split_axis=1, concat_axis=0, tiled=True)
    every_grad = lax.all_gather(logit_grad, "dp", axis=0, tiled=True)
    block_count = owned_cols.shape[0] // tok_rows
    col_blocks = owned_cols.reshape(block_count, tok_rows, row_count)
    grad_blocks = every_grad.reshape(block_count, tok_rows, shard_width)
    block_terms = jnp.einsum(
        "ntr,ntv->nrv", col_blocks, grad_blocks, preferred_element_type=jnp.float32
    ).astype(jnp.bfloat16)
    weight_grad = jnp.sum(block_terms.astype(jnp.float32), axis=0).astype(jnp.bfloat16)
    return (token_loss, hidden_grad, weight_grad)


def body(hidden, out_weight, targets, token_weight):
    nv = lax.axis_size("vocab")
    nz = nv // 4
    tok = hidden.shape[0]
    rows, width = out_weight.shape
    fits = (
        lax.axis_size("dp") == 2 and nv % 4 == 0 and tok % 32 == 0 and tok % (8 * nz) == 0
        and rows % 768 == 0 and width % 128 == 0
    )
    run = fused_body if fits else plain_body
    return run(hidden, out_weight, targets, token_weight)


def solution(mesh):
    placed = (P("dp", None), P("dp", "vocab"), P("dp"), P("dp"))
    return jax.shard_map(
        body,
        mesh=mesh,
        in_specs=placed,
        out_specs=(P("dp"), P("dp", None), P("dp", "vocab")),
        check_vma=False,
    )
```

```python
import functools

import jax
import jax.numpy as jnp
from jax import lax
from jax.experimental import pallas as pl
from jax.experimental.pallas import tpu as pltpu
from jax.sharding import PartitionSpec as P

softcap = 30.0
MESH = pl.DeviceIdType.MESH
NT = (((1,), (1,)), ((), ()))
TN = (((0,), (0,)), ((), ()))


def kernel(
    nv, nz, vocab_used,
    hidden, weight, targets, token_weight,
    loss_out, hg_out, wg_out,
    w, h, h1, part, part_out, part_in, expo, slope, stat, lg, g_send, g_keep, r1, s2, r2, s3, r3, mine, zb, relay, hg, wg,
    loc_sem, snd_sem, rcv_sem,
):
    tok, rows = h.shape[1], h.shape[2]
    width = w.shape[1]
    grp4 = tok // 4
    grp = tok // nz
    cols = rows // 2
    x = lax.axis_index("dp")
    v = lax.axis_index("vocab")
    z, y, core = v // 4, (v // 2) % 2, v % 2
    ox, oy, oc = 1 - x, 1 - y, 1 - core

    def vid(zz, yy, cc):
        return zz * 4 + yy * 2 + cc

    peer_x = (ox, v)
    peer_c = (x, vid(z, y, oc))
    peer_y = (x, vid(z, oy, core))

    def remote(src, dst, sem, dev, rsem=None):
        return pltpu.make_async_remote_copy(
            src_ref=src, dst_ref=dst, send_sem=snd_sem.at[sem],
            recv_sem=rcv_sem.at[sem if rsem is None else rsem],
            device_id=dev, device_id_type=MESH,
        )

    A_X, A_Y, A_C, A_CY, B0, LG, C0 = 0, 1, 2, 3, 4, 8, 9
    R1 = C0 + nv
    R2 = R1 + 2 * nz
    R3 = R2 + 2 * nz
    Z0 = R3 + 2 * nz
    X0 = Z0 + 2 * nz
    Y0 = X0 + 2 * nz
    K0 = Y0 + 2 * nz

    first = -(-(cols // 128) // 2) * 128
    parts = [pl.ds(0, first), pl.ds(first, cols - first)]

    own_cols = pl.ds(pl.multiple_of(x * rows, 128), rows)
    oth_cols = pl.ds(pl.multiple_of(ox * rows, 128), rows)
    ld_h = pltpu.make_async_copy(hidden.at[:, own_cols], h.at[0], loc_sem.at[0])
    ld_w = pltpu.make_async_copy(weight, w, loc_sem.at[1])
    ld_h.start()
    ld_w.start()

    barrier = pltpu.get_barrier_semaphore()
    pl.semaphore_signal(barrier, inc=1, device_id=peer_x, device_id_type=MESH)
    for j in range(1, nv):
        pl.semaphore_signal(barrier, inc=1, device_id=(x, (v + j) % nv), device_id_type=MESH)
    pl.semaphore_wait(barrier, nv)

    def piece(yy, cc):
        return h1.at[2 * yy + cc]

    q = 2 * y + core
    a_x = remote(
        hidden.at[pl.ds(pl.multiple_of(q * grp4, 8), grp4), oth_cols], piece(y, core), A_X, peer_x
    )
    a_x.start()
    ld_h.wait()
    ld_w.wait()
    part[...] = jnp.dot(h[0], w[...], preferred_element_type=jnp.float32)
    a_x.wait_recv()
    a_y = remote(piece(y, core), piece(y, core), A_Y, peer_y)
    a_y.start()
    a_c = remote(piece(y, core), piece(y, core), A_C, peer_c)
    a_c.start()
    sends = [a_x, a_y, a_c]
    bs = []

    def send_part(n, yy, cc):
        i = 2 * yy + cc
        part_out[i] = jnp.dot(h1[i], w[...], preferred_element_type=jnp.float32)
        c = remote(part_out.at[i], part_in.at[i], B0 + n, peer_x)
        c.start()
        bs.append(c)

    send_part(0, y, core)
    remote(piece(y, oc), piece(y, oc), A_C, peer_c).wait_recv()
    send_part(1, y, oc)
    remote(piece(oy, core), piece(oy, core), A_Y, peer_y).wait_recv()
    a_cy = remote(piece(oy, core), piece(oy, core), A_CY, peer_c)
    a_cy.start()
    sends.append(a_cy)
    send_part(2, oy, core)
    remote(piece(oy, oc), piece(oy, oc), A_CY, peer_c).wait_recv()
    send_part(3, oy, oc)
    sends += bs
    for c in bs:
        c.wait_recv()

    def column(ref):
        row = ref[...].reshape(1, tok)
        row = jnp.concatenate([row, jnp.zeros((1, stat.shape[2] - tok), row.dtype)], axis=1)
        return jnp.broadcast_to(row, (128, stat.shape[2])).T[:tok, 0:1]

    target_col, weight_col = column(targets), column(token_weight)
    col_ids = v * width + lax.broadcasted_iota(jnp.int32, (grp4, width), 1)
    lane = lax.broadcasted_iota(jnp.int32, (grp4, 128), 1)
    stats = []
    for i in range(4):
        sl = slice(i * grp4, (i + 1) * grp4)
        squash = jnp.tanh((part[sl] + part_in[i]) / softcap)
        capped = softcap * squash
        e = jnp.where(col_ids < vocab_used, jnp.exp(capped), 0.0)
        hit = col_ids == target_col[sl]
        expo[sl] = e
        slope[sl] = 1.0 - squash * squash
        s_col = jnp.sum(e, axis=1, keepdims=True)
        t_col = jnp.sum(jnp.where(hit, capped, 0.0), axis=1, keepdims=True)
        stats.append(jnp.where(lane == 0, s_col, jnp.where(lane == 1, t_col, 0.0)))
    pad = jnp.zeros((stat.shape[2] - tok, 128), jnp.float32)
    stat[v] = jnp.concatenate(stats + [pad], axis=0).T[:8]
    for j in range(1, nv):
        c = remote(stat.at[v], stat.at[v], C0 + j, (x, (v + j) % nv))
        c.start()
        sends.append(c)
    for j in range(1, nv):
        src = (v + nv - j) % nv
        remote(stat.at[src], stat.at[src], C0 + j, (x, src)).wait_recv()
    total = stat[0]
    for i in range(1, nv):
        total = total + stat[i]
    loss_out[...] = total[0:2, :tok]
    grads = []
    wide = jnp.concatenate([total] + [jnp.zeros_like(total)] * 15, axis=0).T
    for i in range(4):
        sl = slice(i * grp4, (i + 1) * grp4)
        hit = col_ids == target_col[sl]
        onehot = jnp.where(hit, jnp.float32(1.0), jnp.float32(0.0))
        grads.append(weight_col[sl] * (expo[sl] / wide[sl, 0:1] - onehot) * slope[sl])
    lg[0] = jnp.concatenate(grads, axis=0).astype(jnp.bfloat16)
    lg_x = remote(lg.at[0], lg.at[1], LG, peer_x)
    lg_x.start()
    sends.append(lg_x)

    step = cols // 3
    r1s = []
    for d in range(2):
        if d == 1:
            lg_x.wait_recv()
        tk = x if d == 0 else ox
        g = lg[d]
        for n in range(3):
            wr = w[pl.ds(pl.multiple_of(oc * cols + n * step, 16), step)]
            o = lax.dot_general(g, wr, NT, preferred_element_type=jnp.float32)
            for k in range(nz):
                g_send[tk, k, :, n * step:(n + 1) * step] = o[k * grp:(k + 1) * grp].astype(jnp.bfloat16)
        for k in range(nz):
            c = remote(g_send.at[tk, k], r1.at[tk, k], R1 + tk * nz + k, peer_c)
            c.start()
            r1s.append(c)
        for n in range(3):
            wr = w[pl.ds(pl.multiple_of(core * cols + n * step, 16), step)]
            o = lax.dot_general(g, wr, NT, preferred_element_type=jnp.float32)
            for k in range(nz):
                g_keep[tk, k, :, n * step:(n + 1) * step] = o[k * grp:(k + 1) * grp]
    sends += r1s

    def from_partner(d, k):
        remote(r1.at[d, k], r1.at[d, k], R1 + d * nz + k, peer_c).wait_recv()

    r2s = []
    for p, cs in enumerate(parts):
        for j in range(nz):
            k = (z + 1 + j) % nz
            if p == 0:
                from_partner(oy, k)
            s2[k, :, cs] = (g_keep[oy, k, :, cs] + r1[oy, k, :, cs].astype(jnp.float32)).astype(
                jnp.bfloat16
            )
            c = remote(s2.at[k, :, cs], r2.at[k, :, cs], R2 + p * nz + j, peer_y)
            c.start()
            r2s.append(c)
    sends += r2s

    wstep = rows // 6
    for i in range(4):
        h[1, i * grp4:(i + 1) * grp4] = h1[i]

    def weight_part(n):
        cs = slice(n * wstep, (n + 1) * wstep)
        o0 = lax.dot_general(h[0, :, cs], lg[0], TN, preferred_element_type=jnp.float32)
        o1 = lax.dot_general(h[1, :, cs], lg[1], TN, preferred_element_type=jnp.float32)
        o0 = o0.astype(jnp.bfloat16).astype(jnp.float32)
        o1 = o1.astype(jnp.bfloat16).astype(jnp.float32)
        wg[cs] = (o0 + o1).astype(jnp.bfloat16)

    r3s = []
    for p, cs in enumerate(parts):
        for j in range(nz):
            k = (z + 1 + j) % nz
            if p == 0:
                from_partner(y, k)
            r2s[p * nz + j].wait_recv()
            t = (
                g_keep[y, k, :, cs]
                + r1[y, k, :, cs].astype(jnp.float32)
                + r2[k, :, cs].astype(jnp.float32)
            )
            if j < nz - 1:
                s3[k, :, cs] = t.astype(jnp.bfloat16)
                c = remote(
                    s3.at[k, :, cs], r3.at[j, :, cs], R3 + p * nz + j, (x, vid(k, y, core))
                )
                c.start()
                r3s.append(c)
            else:
                mine[:, cs] = t
        if p == 0:
            for n in range(3):
                weight_part(n)
    sends += r3s

    zs = []
    for p, cs in enumerate(parts):
        t = mine[:, cs]
        for j in range(nz - 1):
            r3s[p * (nz - 1) + j].wait_recv()
            t = t + r3[j, :, cs].astype(jnp.float32)
        zb[z, :, cs] = t.astype(jnp.bfloat16)
        for j in range(nz - 1):
            k = (z + 1 + j) % nz
            c = remote(zb.at[z, :, cs], zb.at[z, :, cs], Z0 + p * nz + j, (x, vid(k, y, core)))
            c.start()
            zs.append(c)
        if p == 0:
            for n in range(3, 6):
                weight_part(n)
            st_w = pltpu.make_async_copy(wg, wg_out, loc_sem.at[2])
            st_w.start()
    sends += zs

    def fan(p, k, j):
        cs, i = parts[p], p * nz + j
        src, dst = zb.at[k, :, cs], hg.at[x, core, k, :, cs]
        hop = relay.at[k, :, cs]
        return (
            remote(src, dst, Y0 + i, peer_y),
            remote(hop, dst, X0 + i, peer_x),
            remote(src, dst, X0 + i, peer_x),
            remote(src, hop, Y0 + i, peer_y),
        )

    def relay_on(p, k, j):
        @pl.when(x == y)
        def _():
            hop = relay.at[k, :, parts[p]]
            remote(hop, hop, Y0 + p * nz + j, peer_y).wait_recv()
            fan(p, k, j)[1].start()

    for p, cs in enumerate(parts):
        for j in range(nz):
            k = (z + nz - j) % nz
            if j:
                remote(
                    zb.at[k, :, cs], zb.at[k, :, cs], Z0 + p * nz + j - 1, (x, vid(k, y, core))
                ).wait_recv()
            home_y, home_x, away_x, away_y = fan(p, k, j)

            @pl.when(x == y)
            def _():
                home_y.start()
                hg[x, core, k, :, cs] = zb[k, :, cs]

            @pl.when(x != y)
            def _():
                away_y.start()
                away_x.start()

            if j or p:
                relay_on(*last)
            last = (p, k, j)
    relay_on(*last)

    ks = []
    for p, cs in enumerate(parts):
        for j in range(nz):
            k = (z + nz - j) % nz
            i = p * nz + j

            @pl.when(x != y)
            def _():
                spot = hg.at[x, core, k, :, cs]
                remote(spot, spot, Y0 + i, peer_y).wait_recv()

            spot = hg.at[ox, core, k, :, cs]
            remote(spot, spot, X0 + i, peer_x).wait_recv()

            for xs in range(2):
                spot = hg.at[xs, core, k, :, cs]
                c = remote(spot, spot, K0 + 2 * i + xs, peer_c)
                c.start()
                ks.append(c)
    sends += ks

    outs = []

    def put(cc, xs, k, n):
        c = pltpu.make_async_copy(
            hg.at[xs, cc, k],
            hg_out.at[
                pl.ds(pl.multiple_of(k * grp, 8), grp),
                pl.ds(pl.multiple_of(xs * rows + cc * cols, 128), cols),
            ],
            loc_sem.at[3 + n],
        )
        c.start()
        outs.append(c)

    for j in range(nz):
        k = (z + nz - j) % nz
        for xs in range(2):
            put(core, xs, k, 4 * j + xs)
    for j in range(nz):
        k = (z + nz - j) % nz
        for xs in range(2):
            for p, cs in enumerate(parts):
                spot = hg.at[xs, oc, k, :, cs]
                remote(spot, spot, K0 + 2 * (p * nz + j) + xs, peer_c).wait_recv()
            put(oc, xs, k, 4 * j + 2 + xs)

    for c in sends:
        c.wait_send()
    for p in range(2):
        for j in range(nz):
            home_y, home_x, away_x, away_y = fan(p, (z + nz - j) % nz, j)

            @pl.when(x == y)
            def _():
                home_y.wait_send()
                home_x.wait_send()

            @pl.when(x != y)
            def _():
                away_y.wait_send()
                away_x.wait_send()

    st_w.wait()
    for c in outs:
        c.wait()


def fused_body(hidden, out_weight, targets, token_weight):
    nv = lax.axis_size("vocab")
    nz = nv // 4
    tok = hidden.shape[0]
    rows, width = out_weight.shape
    grp, cols = tok // nz, rows // 2
    lanes = -(-tok // 128) * 128
    bf, f32 = jnp.bfloat16, jnp.float32
    anyspec = pl.BlockSpec(memory_space=pl.ANY)
    vspec = pl.BlockSpec(memory_space=pltpu.VMEM)
    nsem = 9 + nv + 16 * nz
    loss, hg, wg = pl.pallas_call(
        functools.partial(kernel, nv, nz, width * nv - width // 2),
        out_shape=(
            jax.ShapeDtypeStruct((2, tok), f32),
            jax.ShapeDtypeStruct((tok, 2 * rows), bf),
            jax.ShapeDtypeStruct((rows, width), bf),
        ),
        in_specs=[anyspec, anyspec, vspec, vspec],
        out_specs=(vspec, anyspec, anyspec),
        scratch_shapes=[
            pltpu.VMEM((rows, width), bf),
            pltpu.VMEM((2, tok, rows), bf),
            pltpu.VMEM((4, tok // 4, rows), bf),
            pltpu.VMEM((tok, width), f32),
            pltpu.VMEM((4, tok // 4, width), f32),
            pltpu.VMEM((4, tok // 4, width), f32),
            pltpu.VMEM((tok, width), f32),
            pltpu.VMEM((tok, width), f32),
            pltpu.VMEM((nv, 8, lanes), f32),
            pltpu.VMEM((2, tok, width), bf),
            pltpu.VMEM((2, nz, grp, cols), bf),
            pltpu.VMEM((2, nz, grp, cols), f32),
            pltpu.VMEM((2, nz, grp, cols), bf),
            pltpu.VMEM((nz, grp, cols), bf),
            pltpu.VMEM((nz, grp, cols), bf),
            pltpu.VMEM((nz, grp, cols), bf),
            pltpu.VMEM((nz, grp, cols), bf),
            pltpu.VMEM((grp, cols), f32),
            pltpu.VMEM((nz, grp, cols), bf),
            pltpu.VMEM((nz, grp, cols), bf),
            pltpu.VMEM((2, 2, nz, grp, cols), bf),
            pltpu.VMEM((rows, width), bf),
            pltpu.SemaphoreType.DMA((3 + 4 * nz,)),
            pltpu.SemaphoreType.DMA((nsem,)),
            pltpu.SemaphoreType.DMA((nsem,)),
        ],
        compiler_params=pltpu.CompilerParams(
            collective_id=0, has_side_effects=True, vmem_limit_bytes=56 * 1024 * 1024
        ),
    )(hidden, out_weight, targets, token_weight)
    return jnp.log(loss[0]) - loss[1], hg, wg


def plain_body(hidden, out_weight, targets, token_weight):
    shard_width = out_weight.shape[1]
    row_count = out_weight.shape[0]
    tok_rows = hidden.shape[0]
    vocab_used = shard_width * lax.axis_size("vocab") - shard_width // 2
    first_col = lax.axis_index("vocab") * shard_width
    col_ids = first_col + jnp.arange(shard_width, dtype=jnp.int32)
    usable = col_ids < vocab_used
    w_full = lax.all_gather(out_weight, "dp", axis=0, tiled=True)
    logits = jnp.dot(hidden, w_full, preferred_element_type=jnp.float32)
    squash = jnp.tanh(logits / softcap)
    capped = softcap * squash
    exp_terms = jnp.where(usable[None, :], jnp.exp(capped), jnp.float32(0.0))
    target_hit = col_ids[None, :] == targets[:, None]
    local_sum = jnp.sum(exp_terms, axis=1)
    local_target = jnp.sum(jnp.where(target_hit, capped, jnp.float32(0.0)), axis=1)
    sums, target_logit = lax.psum((local_sum, local_target), "vocab")
    token_loss = jnp.log(sums) - target_logit
    onehot = jnp.where(target_hit, jnp.float32(1.0), jnp.float32(0.0))
    logit_grad = (
        token_weight[:, None] * (exp_terms / sums[:, None] - onehot) * (1.0 - squash * squash)
    ).astype(jnp.bfloat16)
    partial_grad = lax.dot_general(logit_grad, w_full, NT, preferred_element_type=jnp.float32)
    share = lax.psum_scatter(partial_grad, "vocab", scatter_dimension=1, tiled=True).astype(
        jnp.bfloat16
    )
    hidden_grad = lax.all_gather(share, "vocab", axis=1, tiled=True)
    owned_cols = lax.all_to_all(hidden, "dp", split_axis=1, concat_axis=0, tiled=True)
    every_grad = lax.all_gather(logit_grad, "dp", axis=0, tiled=True)
    block_count = owned_cols.shape[0] // tok_rows
    col_blocks = owned_cols.reshape(block_count, tok_rows, row_count)
    grad_blocks = every_grad.reshape(block_count, tok_rows, shard_width)
    block_terms = jnp.einsum(
        "ntr,ntv->nrv", col_blocks, grad_blocks, preferred_element_type=jnp.float32
    ).astype(jnp.bfloat16)
    weight_grad = jnp.sum(block_terms.astype(jnp.float32), axis=0).astype(jnp.bfloat16)
    return (token_loss, hidden_grad, weight_grad)


def body(hidden, out_weight, targets, token_weight):
    nv = lax.axis_size("vocab")
    nz = nv // 4
    tok = hidden.shape[0]
    rows, width = out_weight.shape
    fits = (
        lax.axis_size("dp") == 2 and nv % 4 == 0 and tok % 32 == 0 and tok % (8 * nz) == 0
        and rows % 768 == 0 and width % 128 == 0
    )
    run = fused_body if fits else plain_body
    return run(hidden, out_weight, targets, token_weight)


def solution(mesh):
    placed = (P("dp", None), P("dp", "vocab"), P("dp"), P("dp"))
    return jax.shard_map(
        body,
        mesh=mesh,
        in_specs=placed,
        out_specs=(P("dp"), P("dp", None), P("dp", "vocab")),
        check_vma=False,
    )
```
